256 devices in a mesh: dp: 2 (over core), seq: 32 (over z, x), mp: 4 (over y).
Axes of the slice: x: 4, y: 4, z: 8, core: 2. Of those that a mesh axis runs over, the one named last changes fastest.
Arguments:
- queries: bfloat16 [6, 4096, 4096], P('dp', 'seq', 'mp'), may hold values from -1000 to 1000
- database: bfloat16 [1024, 128, 1024], P('seq', None, 'mp'), may hold values from -300 to 300
- owner_ids: int32 [2, 32, 6, 2], P('dp'), may hold values from 0 to 31, all different within a row; in each aligned block of 6 rows (0 to 5, 6 to 11, ..., all dimensions but the last counted through in order) at most 2 rows name the same one
- row_ids: int32 [2, 32, 6, 2], P('dp'), may hold values from 0 to 31
- pre_gain: float32 [1024], replicated, may hold values from 0.1 to 1.9
- out_gain: float32 [1024], replicated, may hold values from 0.1 to 1.9
- w_in: bfloat16 [1024, 4096], P(None, 'mp'), may hold values from -0.1875 to 0.1875
- w_out: bfloat16 [4096, 1024], P('mp'), may hold values from -0.09375 to 0.09375
- w_key: bfloat16 [1024, 4096], P(None, 'mp'), may hold values from -0.1875 to 0.1875
- w_value: bfloat16 [1024, 4096], P(None, 'mp'), may hold values from -0.1875 to 0.1875
Outputs:
- attended: bfloat16 [6, 4096, 4096], P('dp', 'seq', 'mp')
The draws below stay inside these ranges and needn't reach their ends.
Inputs may be any that keep to these rules, and one draw needn't show every extreme that they name: `owner_ids`: within one index pair of the first two dimensions (the 6 spans of one device) no shard number appears more than 2 times, and the 2 neighbours of one span lie on different shards.
All inputs are finite; a program needn't handle non-finite values.
Results may differ from the reference program's by a relative error of at most 0.04.
Values may be sent and summed in bfloat16 or wider, within the bound.
No kernel may reach another device: no remote copies, remote signals or barrier semaphores. Data moves between devices by JAX's collectives and lax.ppermute only.
A program may use at most 64 MiB of HBM per device.

```python
import math
import jax
import jax.numpy as jnp
import numpy as np
from jax import lax

HEADS = 32
HD = 128
E = 1024
FF_ENC = 4096
SPAN = 64
RLEN = 128
NEIGH = 2
MOST = 2
SEQS = 3
CH_DEV = 2
DB_DEV = 32
D = 4096
SPANS = 64
LENGTH = 4096
BATCH = 6
ENTRIES = 1024
N_DP = 2
N_SEQ = 32
N_MP = 4


def draw_queries(key, part):
    key_base = jax.random.fold_in(jax.random.fold_in(key, 11), 0)
    full_shape = (BATCH, LENGTH, D)
    values = 2.0 * jnp.clip(jax.random.normal(key_base, full_shape, jnp.float32), -6.0, 6.0)
    return values.astype(jnp.bfloat16)


def draw_database(key, part):
    key_base = jax.random.fold_in(jax.random.fold_in(key, 23), 0)
    full_shape = (ENTRIES, RLEN, E)
    values = jnp.clip(jax.random.normal(key_base, full_shape, jnp.float32), -6.0, 6.0)
    return values.astype(jnp.bfloat16)


def with_ends(values, key, least, top_value):
    shape = values.shape
    place = [jax.random.randint(jax.random.fold_in(key, axis), (), 0, shape[axis]) for axis in range(len(shape))]
    values = values.at[tuple(place)].set(least)
    longest = shape.index(max(shape))
    place[longest] = (place[longest] + 1) % shape[longest]
    return values.at[tuple(place)].set(top_value)


def shard_levels(own_key, dims, cuts, smallest, top_value):
    def one(dim, blocks):
        steps = jax.random.uniform(jax.random.fold_in(jax.random.fold_in(own_key, 6), dim), (blocks,), jnp.float32, smallest / len(cuts), top_value / len(cuts))
        return jnp.repeat(jnp.exp(steps), dims[dim] // blocks).reshape((-1,) + (1,) * (len(dims) - dim - 1))

    gain = one(*cuts[0])
    for cut in cuts[1:]:
        gain = gain * one(*cut)
    return gain


def deal_out(rng, own, number, rows, number_of, top, most, lean):
    sequence = jax.random.permutation(rng, number_of)
    heavy_load, ordinary = portions_of(number_of, rows * top, most, lean, True), portions_of(number_of, rows * top, most, lean, False)
    places = jnp.arange(number_of)

    def named(lengths, offset_by):
        used = int((lengths > 0).sum())
        fixed = max(1, used // 4)
        passed = fixed + (places - fixed + offset_by * (used - fixed)) % max(1, number_of - fixed)
        return jnp.zeros((number_of,), jnp.int32).at[sequence[jnp.where(places < fixed, places, passed)]].set(jnp.asarray(lengths, jnp.int32))

    lengths = jnp.where(number % 4 == 0, named(heavy_load, number // 4), named(ordinary, number - number // 4 - 1))
    mixed = jax.random.permutation(jax.random.fold_in(own, 3), number_of)
    giver, sink = mixed[0:number_of // 2 * 2:2], mixed[1:number_of // 2 * 2:2]
    room = jnp.minimum(lengths[giver] - 1, most - lengths[sink]) // 2
    room = jnp.where((giver == sequence[0]) | (sink == sequence[0]) | (lengths[sink] == 0), 0, jnp.maximum(room, 0))
    passed = jax.random.randint(jax.random.fold_in(own, 4), (number_of // 2,), 0, 1 << 20) % (room + 1)
    lengths = lengths.at[giver].add(-passed).at[sink].add(passed)
    items = jnp.searchsorted(jnp.cumsum(lengths), jnp.arange(rows * top), side="right").astype(jnp.int32)
    grid = items.reshape(top, rows).T
    grid = grid[jax.random.permutation(jax.random.fold_in(own, 1), rows)]
    offset_by = jax.random.randint(jax.random.fold_in(own, 2), (rows, 1), 0, top)
    return jnp.take_along_axis(grid, (jnp.arange(top)[None, :] + offset_by) % top, axis=1)


def portions_of(amount, total, limit, slope, full):
    weights = [(1 << 20) // math.isqrt(grade ** slope) + 1 for grade in range(1, amount + 1)]
    largest = limit if full else min(limit, max(-(-total // amount), total * weights[0] // sum(weights)))
    least = 1 if total - largest >= amount - 1 else 0
    holding, surplus = [largest] + [least] * (amount - 1), total - largest - least * (amount - 1)
    while surplus > 0:
        free = [i for i in range(1, amount) if holding[i] < largest] or [i for i in range(1, amount) if holding[i] < limit]
        whole, remaining = sum([weights[i] for i in free]), surplus
        for i in free:
            extra = min(limit - holding[i], max(1, remaining * weights[i] // whole), surplus)
            holding[i] = holding[i] + extra
            surplus = surplus - extra
    return np.array(holding)


def gaussian(own_key, extent, scale, most, cuts=(), held_as=jnp.bfloat16):
    values = jax.random.normal(own_key, extent, jnp.float32) * scale
    if len(cuts) > 0:
        values = shard_levels(own_key, extent, cuts, -0.22, 0.18) * values
    return jnp.clip(values, min=-most, max=most).astype(held_as)


def setup_inputs(seed: int = 0) -> dict:
    streams_of = jax.random.split(jax.random.key(seed), 11)
    queries = draw_queries(jax.random.fold_in(streams_of[10], 71), 0)
    database = draw_database(jax.random.fold_in(streams_of[10], 71), 0)
    owner_ids_keys = jax.random.split(jax.random.fold_in(streams_of[2], 1), N_DP * N_SEQ * (SEQS * CH_DEV) // (SEQS * CH_DEV))
    owner_ids_turns = jax.random.permutation(jax.random.fold_in(streams_of[2], 3), N_DP * N_SEQ * (SEQS * CH_DEV) // (SEQS * CH_DEV))
    owner_ids = jax.vmap(lambda own, number: deal_out(jax.random.fold_in(streams_of[2], 2), own, number, SEQS * CH_DEV, N_SEQ, NEIGH, MOST, 2))(owner_ids_keys, owner_ids_turns).reshape((N_DP, N_SEQ, SEQS * CH_DEV, NEIGH))
    row_ids = with_ends(jax.random.randint(streams_of[3], (N_DP, N_SEQ, SEQS * CH_DEV, NEIGH), 0, DB_DEV), jax.random.fold_in(streams_of[3], 1), 0, DB_DEV - 1).astype(jnp.int32)
    pre_gain = jnp.clip(1.0 + 0.18 * jax.random.normal(streams_of[4], (E,), jnp.float32), 0.1, 1.9)
    out_gain = jnp.clip(1.0 + 0.18 * jax.random.normal(streams_of[5], (E,), jnp.float32), 0.1, 1.9)
    w_in = gaussian(streams_of[6], (E, FF_ENC), E ** -0.5, 0.1875, ((1, 4),))
    w_out = gaussian(streams_of[7], (FF_ENC, E), FF_ENC ** -0.5, 0.09375, ((0, 4),))
    w_key = gaussian(streams_of[8], (E, D), E ** -0.5, 0.1875, ((1, 4),))
    w_value = gaussian(streams_of[9], (E, D), E ** -0.5, 0.1875, ((1, 4),))
    return dict(queries=queries, database=database, owner_ids=owner_ids, row_ids=row_ids, pre_gain=pre_gain, out_gain=out_gain, w_in=w_in, w_out=w_out, w_key=w_key, w_value=w_value)


epsilon = 1e-06

def rms_scale(values, gain_values):
    return values * lax.rsqrt(lax.optimization_barrier(jnp.mean(values * values, axis=-1, keepdims=True)) + epsilon) * gain_values

def arrange(index_table):
    index_table = index_table.reshape(N_DP, N_SEQ, SEQS, CH_DEV, NEIGH).transpose(0, 2, 1, 3, 4)
    return index_table.reshape(BATCH, SPANS, NEIGH).astype(jnp.int32)

def reference(queries, database, owner_ids, row_ids, pre_gain, out_gain, w_in, w_out, w_key, w_value):
    entries = arrange(owner_ids) * DB_DEV + arrange(row_ids)
    group_width = FF_ENC // N_MP

    def one_sequence(inputs):
        query_rows, entry_rows = inputs
        blocks = jnp.take(database, entry_rows[:-1].reshape(-1), axis=0)
        widened = blocks.reshape(-1, E).astype(jnp.float32)
        normed = rms_scale(widened, pre_gain).astype(jnp.bfloat16)
        hidden_act = jax.nn.gelu(jnp.dot(normed, w_in, preferred_element_type=jnp.float32)).astype(jnp.bfloat16)
        summed = jnp.zeros(widened.shape, jnp.float32)
        for part_index in range(N_MP):
            lower = part_index * group_width
            partial_sum = jnp.dot(hidden_act[:, lower:lower + group_width], w_out[lower:lower + group_width], preferred_element_type=jnp.float32)
            summed = summed + lax.optimization_barrier(partial_sum.astype(jnp.bfloat16)).astype(jnp.float32)
        encoded = rms_scale(widened + summed, out_gain).astype(jnp.bfloat16)
        key_rows = jnp.dot(encoded, w_key, preferred_element_type=jnp.float32).astype(jnp.bfloat16)
        value_rows = jnp.dot(encoded, w_value, preferred_element_type=jnp.float32).astype(jnp.bfloat16)
        key_rows = key_rows.reshape(SPANS - 1, NEIGH * RLEN, HEADS, HD).astype(jnp.float32)
        value_rows = value_rows.reshape(SPANS - 1, NEIGH * RLEN, HEADS, HD).astype(jnp.float32)
        query_part = query_rows.reshape(SPANS, SPAN, HEADS, HD)[1:].astype(jnp.float32)
        scores = jnp.einsum('cqhd,ckhd->chqk', query_part, key_rows, precision=lax.Precision.HIGHEST) * HD ** (-0.5)
        scores = scores - lax.optimization_barrier(jnp.max(scores, axis=-1, keepdims=True))
        weights = jnp.exp(scores)
        weights = (weights / lax.optimization_barrier(jnp.sum(weights, axis=-1, keepdims=True))).astype(jnp.bfloat16).astype(jnp.float32)
        attended = jnp.einsum('chqk,ckhd->cqhd', weights, value_rows, precision=lax.Precision.HIGHEST)
        attended = jnp.concatenate([jnp.zeros((1, SPAN, HEADS, HD), jnp.float32), attended], axis=0)
        return attended.reshape(LENGTH, D).astype(jnp.bfloat16)
    return lax.map(one_sequence, (queries, entries))
```

```python
import functools
import jax
import jax.numpy as jnp
from jax import lax
from jax.experimental import pallas as pl
from jax.experimental.pallas import tpu as pltpu
from jax.sharding import PartitionSpec as P

HD = 128
MOST = 2
CHUNKS = ((0, 64), (64, 64))
EPS = 1e-06
VMEM_LIMIT = 56 * 1024 * 1024


def vmem():
    return pl.BlockSpec(memory_space=pltpu.VMEM)


def smem():
    return pl.BlockSpec(memory_space=pltpu.SMEM)


def anywhere():
    return pl.BlockSpec(memory_space=pl.ANY)


def cost(flops, moved):
    return pl.CostEstimate(flops=int(flops), bytes_accessed=int(moved), transcendentals=0)


def moved_by(array, axis, by, wrap=True):
    peers = lax.axis_size(axis)
    pairs = [(i, (i + by) % peers) for i in range(peers) if wrap or 0 <= i + by < peers]
    return lax.ppermute(array, axis, pairs)


def pack_kernel(me_ref, owners_ref, rows_ref, db_ref, *outs):
    me = me_ref[0]
    slots, neigh, shards = owners_ref.shape

    def one(r, carry):
        count = jnp.int32(0)
        first = jnp.int32(0)
        second = jnp.int32(0)
        for j in range(slots):
            for n in range(neigh):
                hit = owners_ref[j, n, r] == me
                row = rows_ref[j, n, r]
                first = jnp.where(hit & (count == 0), row, first)
                second = jnp.where(hit & (count == 1), row, second)
                count = count + hit.astype(jnp.int32)
        for rank, row in enumerate((first, second)):
            for (start, size), out in zip(CHUNKS, outs):
                out[r * MOST + rank] = db_ref[row, start : start + size, :]
        return carry

    lax.fori_loop(0, shards, one, 0)


def pack(me, owners, rows, database):
    shards = owners.shape[2]
    width = database.shape[2]
    return pl.pallas_call(
        pack_kernel,
        out_shape=[
            jax.ShapeDtypeStruct((shards * MOST, size, width), database.dtype)
            for _, size in CHUNKS
        ],
        in_specs=[smem(), smem(), smem(), vmem()],
        out_specs=[vmem() for _ in CHUNKS],
        compiler_params=pltpu.CompilerParams(vmem_limit_bytes=VMEM_LIMIT),
        cost_estimate=cost(1e9, 6e6),
        name="pack",
    )(me, owners, rows, database)


def pick_kernel(parts, me_ref, owners_ref, arrived_ref, out_ref, sems):
    me = me_ref[0]
    slots, neigh, _ = owners_ref.shape
    part_rows = out_ref.shape[3]
    wanted = [owners_ref[j, n, me] for j in range(slots) for n in range(neigh)]
    copies = []
    for i, owner in enumerate(wanted):
        rank = jnp.int32(0)
        for other in wanted[:i]:
            rank = rank + (other == owner).astype(jnp.int32)
        slot = owner * MOST + rank
        j, n = i // neigh, i % neigh
        q, c = j // 2, j % 2
        for p in range(parts):
            copies.append(
                pltpu.make_async_copy(
                    arrived_ref.at[slot, pl.ds(p * part_rows, part_rows), :],
                    out_ref.at[p, c, q * neigh + n],
                    sems.at[i * parts + p],
                )
            )
            copies[-1].start()
    for copy in copies:
        copy.wait()


def pick(me, owners, arrived, parts):
    slots, neigh, _ = owners.shape
    _, rows, width = arrived.shape
    return pl.pallas_call(
        functools.partial(pick_kernel, parts),
        out_shape=jax.ShapeDtypeStruct(
            (parts, 2, slots * neigh // 2, rows // parts, width), arrived.dtype
        ),
        in_specs=[smem(), smem(), anywhere()],
        out_specs=vmem(),
        scratch_shapes=[pltpu.SemaphoreType.DMA((slots * neigh * parts,))],
        cost_estimate=cost(2e9, 2e6),
        name="pick",
    )(me, owners, arrived)


def gelu(x):
    inner = 0.7978845608028654 * (x + 0.044715 * (x * x * x))
    return (0.5 * x) * (1.0 + jnp.tanh(inner))


def encode_kernel(n_pieces, x_ref, pre_ref, out_gain_ref, *refs):
    ins = refs[: n_pieces]
    outs = refs[n_pieces : 2 * n_pieces]
    enc0, enc1, win, wout, res, acc, sems = refs[2 * n_pieces :]
    width = win.shape[2]
    plan = []
    for a, b in zip(ins, outs):
        for k in range(a.shape[1] // width):
            plan.append((a.at[:, k * width : (k + 1) * width], b.at[k * width : (k + 1) * width, :]))
    copies = []
    for i, (a, b) in enumerate(plan):
        ca = pltpu.make_async_copy(a, win.at[i], sems.at[0, i])
        cb = pltpu.make_async_copy(b, wout.at[i], sems.at[1, i])
        ca.start()
        cb.start()
        copies.append((ca, cb))
    parts, two, groups, rows, cols = x_ref.shape
    half = groups * rows
    for p in range(parts):
        for c in range(two):
            block = x_ref[p, c].reshape(half, cols)
            res[c * half : (c + 1) * half, p * cols : (p + 1) * cols] = block
    x = res[...].astype(jnp.float32)
    scale = lax.rsqrt(jnp.mean(x * x, axis=-1, keepdims=True) + EPS)
    normed = (x * scale * pre_ref[...]).astype(jnp.bfloat16)
    for i, (ca, cb) in enumerate(copies):
        ca.wait()
        hidden = gelu(jnp.dot(normed, win[i], preferred_element_type=jnp.float32))
        hidden = hidden.astype(jnp.bfloat16)
        cb.wait()
        product = jnp.dot(hidden, wout[i], preferred_element_type=jnp.float32)
        if i == 0:
            acc[...] = product
        else:
            acc[...] += product
    y = res[...].astype(jnp.float32) + acc[...]
    scale = lax.rsqrt(jnp.mean(y * y, axis=-1, keepdims=True) + EPS)
    encoded = (y * scale * out_gain_ref[...]).astype(jnp.bfloat16)
    enc0[...] = encoded[:half]
    enc1[...] = encoded[half:]


def encode(x, pre_gain, out_gain, ins, outs):
    parts, two, groups, rows, cols = x.shape
    half = groups * rows
    total = sum(a.shape[1] for a in ins)
    width = min(a.shape[1] for a in ins)
    features = parts * cols
    n = total // width
    flops = 4 * 2 * half * features * total
    return pl.pallas_call(
        functools.partial(encode_kernel, len(ins)),
        out_shape=[jax.ShapeDtypeStruct((half, features), jnp.bfloat16)] * 2,
        in_specs=[vmem()] * 3 + [anywhere()] * (2 * len(ins)),
        out_specs=[vmem()] * 2,
        scratch_shapes=[
            pltpu.VMEM((n, features, width), jnp.bfloat16),
            pltpu.VMEM((n, width, features), jnp.bfloat16),
            pltpu.VMEM((2 * half, features), jnp.bfloat16),
            pltpu.VMEM((2 * half, features), jnp.float32),
            pltpu.SemaphoreType.DMA((2, n)),
        ],
        compiler_params=pltpu.CompilerParams(vmem_limit_bytes=VMEM_LIMIT),
        cost_estimate=cost(flops, 4 * features * total),
        name="encode",
    )(x, pre_gain.reshape(1, -1), out_gain.reshape(1, -1), *ins, *outs)


def keys_kernel(seqs, own, one, three, two_a, two_b, wk, wv, k_ref, v_ref, rows_ref):
    half = two_a.shape[0]
    whole = own.shape[0]
    step = whole // seqs
    gathered = rows_ref.shape[0] // seqs
    pieces = (
        lambda lo, hi: own[lo:hi],
        lambda lo, hi: one[lo:hi],
        lambda lo, hi: three[lo:hi],
    )
    for q in range(seqs):
        base = q * gathered
        for i, piece in enumerate(pieces):
            rows_ref[base + i * step : base + (i + 1) * step] = piece(q * step, (q + 1) * step)
        lo, hi = q * step, (q + 1) * step
        at = base + 3 * step
        if hi <= half:
            rows_ref[at : at + step] = two_a[lo:hi]
        elif lo >= half:
            rows_ref[at : at + step] = two_b[lo - half : hi - half]
        else:
            cut = half - lo
            rows_ref[at : at + cut] = two_a[lo:half]
            rows_ref[at + cut : at + step] = two_b[0 : hi - half]
    rows = rows_ref[...]
    for w, out in ((wk, k_ref), (wv, v_ref)):
        out[...] = jnp.dot(rows, w[...], preferred_element_type=jnp.float32).astype(jnp.bfloat16)


def keys_values(pieces, wk, wv, seqs):
    whole, features = pieces[0].shape
    width = wk.shape[1]
    rows = 4 * whole
    return pl.pallas_call(
        functools.partial(keys_kernel, seqs),
        out_shape=[jax.ShapeDtypeStruct((rows, width), jnp.bfloat16)] * 2,
        in_specs=[vmem()] * 7,
        out_specs=[vmem()] * 2,
        scratch_shapes=[pltpu.VMEM((rows, features), jnp.bfloat16)],
        compiler_params=pltpu.CompilerParams(vmem_limit_bytes=VMEM_LIMIT),
        cost_estimate=cost(4 * rows * features * width, 8e6),
        name="keys",
    )(*pieces, wk, wv)


def attend_kernel(n_chunks, live_ref, q_ref, *refs):
    out_ref = refs[-1]
    span = q_ref.shape[1] // 2
    scale = HD ** (-0.5)
    dims_t = (((1,), (1,)), ((), ()))
    for c in range(2):
        ks = refs[c * 2 * n_chunks : c * 2 * n_chunks + n_chunks]
        vs = refs[c * 2 * n_chunks + n_chunks : (c + 1) * 2 * n_chunks]
        for h in range(q_ref.shape[2] // HD):
            cols = slice(h * HD, (h + 1) * HD)
            q = q_ref[0, c * span : (c + 1) * span, cols]
            scores = [
                lax.dot_general(q, k[0, :, cols], dims_t, preferred_element_type=jnp.float32) * scale
                for k in ks
            ]
            top = functools.reduce(
                jnp.maximum, [jnp.max(s, axis=-1, keepdims=True) for s in scores]
            )
            weights = [jnp.exp(s - top) for s in scores]
            total = functools.reduce(
                jnp.add, [jnp.sum(w, axis=-1, keepdims=True) for w in weights]
            )
            value = functools.reduce(
                jnp.add,
                [
                    jnp.dot(w.astype(jnp.bfloat16), v[0, :, cols], preferred_element_type=jnp.float32)
                    for w, v in zip(weights, vs)
                ],
            )
            value = value / total
            if c == 0:
                value = jnp.where(live_ref[0] > 0, value, 0.0)
            out_ref[0, c * span : (c + 1) * span, cols] = value.astype(out_ref.dtype)


def attend(live, queries, kvs):
    seqs, length, width = queries.shape
    n_chunks = len(kvs[0][0])
    flat = []
    for ks, vs in kvs:
        flat += list(ks) + list(vs)
    return pl.pallas_call(
        functools.partial(attend_kernel, n_chunks),
        grid=(seqs,),
        out_shape=jax.ShapeDtypeStruct(queries.shape, queries.dtype),
        in_specs=[smem(), pl.BlockSpec((1, length, width), lambda i: (i, 0, 0))]
        + [pl.BlockSpec((1,) + a.shape[1:], lambda i: (i, 0, 0)) for a in flat],
        out_specs=pl.BlockSpec((1, length, width), lambda i: (i, 0, 0)),
        compiler_params=pltpu.CompilerParams(vmem_limit_bytes=VMEM_LIMIT),
        cost_estimate=cost(3e9, 8e6),
        name="attend",
    )(live, queries, *flat)


def gather_rows(encoded):
    half = encoded.shape[0] // 2
    one = moved_by(encoded, "mp", 1)
    three = moved_by(encoded, "mp", -1)
    two_a = moved_by(one[:half], "mp", 1)
    two_b = moved_by(three[half:], "mp", -1)
    return encoded, one, three, two_a, two_b


def body(queries, database, owner_ids, row_ids, pre_gain, out_gain, w_in, w_out, w_key, w_value):
    shards = lax.axis_size("seq")
    parts = lax.axis_size("mp")
    me = lax.axis_index("seq")
    core = lax.axis_index("dp")
    seq_count = queries.shape[0]
    hidden = w_in.shape[1] // 2
    a = lax.dynamic_slice_in_dim(w_in, core * hidden, hidden, 1)
    b = lax.dynamic_slice_in_dim(w_out, core * hidden, hidden, 0)
    a1, b3 = moved_by(a, "mp", 1), moved_by(b, "mp", -1)
    a3, b1 = moved_by(a, "mp", -1), moved_by(b, "mp", 1)
    a2, b2 = moved_by(a1, "mp", 1), moved_by(b3, "mp", -1)
    near = (a1, a3, a2), (b1, b3, b2)
    far = [[moved_by(w, "dp", 1) for w in group] for group in near]
    ins = (w_in,) + near[0] + tuple(far[0])
    outs = (w_out,) + near[1] + tuple(far[1])

    owners = owner_ids[0].transpose(1, 2, 0)
    rows = row_ids[0].transpose(1, 2, 0)
    me_array = jnp.reshape(me, (1,)).astype(jnp.int32)
    sent = pack(me_array, owners, rows, database)
    kvs = [([], []), ([], [])]
    for chunk in sent:
        size, width = chunk.shape[1:]
        arrived = lax.all_to_all(
            chunk.reshape(shards, MOST, size, width), "seq", 0, 0, tiled=True
        ).reshape(chunk.shape)
        blocks = pick(me_array, owners, arrived, parts)
        blocks = lax.all_to_all(blocks, "mp", 0, 0, tiled=True)
        here, ahead = encode(blocks, pre_gain, out_gain, ins, outs)
        passed = moved_by(ahead, "seq", 1, wrap=False)
        for c, encoded in ((1, here), (0, passed)):
            k, v = keys_values(gather_rows(encoded), w_key, w_value, seq_count)
            kvs[c][0].append(k.reshape(seq_count, -1, k.shape[-1]))
            kvs[c][1].append(v.reshape(seq_count, -1, v.shape[-1]))
    return attend(me_array, queries, kvs)


def solution(mesh):
    return jax.shard_map(
        body,
        mesh=mesh,
        in_specs=(
            P("dp", "seq", "mp"),
            P("seq", None, "mp"),
            P("dp", None, None, None),
            P("dp", None, None, None),
            P(),
            P(),
            P(None, "mp"),
            P("mp", None),
            P(None, "mp"),
            P(None, "mp"),
        ),
        out_specs=P("dp", "seq", "mp"),
        check_vma=False,
    )
```
